32 devices in a mesh: rep: 2 (over y), exp: 4 (over x, core), tp: 4 (over z).
Axes of the slice: x: 2, y: 2, z: 4, core: 2. Of those that a mesh axis runs over, the one named last changes fastest.
Arguments:
- tokens: bfloat16 [256, 6144], P(('rep', 'exp'), 'tp'), parts along dimension 0, may hold values from -6 to 6
- expert_ids: int32 [256, 2], P(('rep', 'exp')), parts along dimension 0, may hold values from 0 to 3, all different within a row; in each aligned block of 32 rows (0 to 31, 32 to 63, ...) at most 20 rows name the same one
- route_logits: float32 [256, 2], P(('rep', 'exp')), parts along dimension 0, may hold values from -6 to 6
- gate_weight: bfloat16 [6144, 32768], P(None, ('exp', 'tp')), may hold values from -0.078125 to 0.078125
- up_weight: bfloat16 [6144, 32768], P(None, ('exp', 'tp')), may hold values from -0.078125 to 0.078125
- down_weight: bfloat16 [32768, 6144], P(('exp', 'tp')), may hold values from -0.0625 to 0.0625
Outputs:
- moe_out: bfloat16 [256, 6144], P(('rep', 'exp'), 'tp'), parts along dimension 0
The draws below stay inside these ranges and needn't reach their ends.
There are 2 independent parts, one for each index of `rep`. The reference program is written for one: setup_inputs(seed, part) draws one part's arguments, and reference() takes and returns one part's arrays. A program takes and returns all parts, laid end to end along the dimension named above; an argument that names none is the same for every part. Nothing has to cross between parts.
Inputs may be any that keep to these rules, and one draw needn't show every extreme that they name: `expert_ids`: each token names two different experts. In each aligned block of 32 tokens no expert is named by more than 20 tokens, a bound that some block reaches.
All inputs are finite; a program needn't handle non-finite values.
Results may differ from the reference program's by a relative error of at most 0.019.
Values may be sent and summed in bfloat16 or wider, within the bound.
A program may use at most 128 MiB of HBM per device.

```python
import math
import jax
import jax.numpy as jnp
import numpy as np
from jax import lax

D = 6144
FF = 8192
EXPERTS = 4
TOK_EXP = 32
CAP = 20
TOKENS = 128
N_EXP = 4
N_TP = 4


def steps_of(rng, extent, cuts, low, largest):
    gain, own = 1.0, jax.random.fold_in(rng, 6)
    for dim, parts in cuts:
        draws = jnp.exp(jax.random.uniform(jax.random.fold_in(own, dim), (parts,), jnp.float32, low / len(cuts), largest / len(cuts)))
        gain = gain * jnp.repeat(draws, extent[dim] // parts).reshape([-1 if axis == dim else 1 for axis in range(len(extent))])
    return gain


def routed_block(rng, own, number, rows, count, top, bound, lean):
    order = jax.random.permutation(rng, count)
    packed, common = portions_of(count, rows * top, bound, lean, True), portions_of(count, rows * top, bound, lean, False)
    places = jnp.arange(count)

    def named(lengths, rotation):
        used = int((lengths > 0).sum())
        fixed = max(1, used // 4)
        passed = fixed + (places - fixed + rotation * (used - fixed)) % max(1, count - fixed)
        return jnp.zeros((count,), jnp.int32).at[order[jnp.where(places < fixed, places, passed)]].set(jnp.asarray(lengths, jnp.int32))

    lengths = jnp.where(number % 4 == 0, named(packed, number // 4), named(common, number - number // 4 - 1))
    mixed = jax.random.permutation(jax.random.fold_in(own, 3), count)
    source_of, taker = mixed[0:count // 2 * 2:2], mixed[1:count // 2 * 2:2]
    room = jnp.minimum(lengths[source_of] - 1, bound - lengths[taker]) // 2
    room = jnp.where((source_of == order[0]) | (taker == order[0]) | (lengths[taker] == 0), 0, jnp.maximum(room, 0))
    passed = jax.random.randint(jax.random.fold_in(own, 4), (count // 2,), 0, 1 << 20) % (room + 1)
    lengths = lengths.at[source_of].add(-passed).at[taker].add(passed)
    members = jnp.searchsorted(jnp.cumsum(lengths), jnp.arange(rows * top), side="right").astype(jnp.int32)
    listing = members.reshape(top, rows).T
    listing = listing[jax.random.permutation(jax.random.fold_in(own, 1), rows)]
    rotation = jax.random.randint(jax.random.fold_in(own, 2), (rows, 1), 0, top)
    return jnp.take_along_axis(listing, (jnp.arange(top)[None, :] + rotation) % top, axis=1)


def portions_of(number_of, total, reach, skew, full):
    portions = [(1 << 20) // math.isqrt(rank ** skew) + 1 for rank in range(1, number_of + 1)]
    largest = reach if full else min(reach, max(-(-total // number_of), total * portions[0] // sum(portions)))
    least = 1 if total - largest >= number_of - 1 else 0
    counts, spare = [largest] + [least] * (number_of - 1), total - largest - least * (number_of - 1)
    while spare > 0:
        candidates = [i for i in range(1, number_of) if counts[i] < largest] or [i for i in range(1, number_of) if counts[i] < reach]
        pool, remaining = sum([portions[i] for i in candidates]), spare
        for i in candidates:
            more = min(reach - counts[i], max(1, remaining * portions[i] // pool), spare)
            counts[i] = counts[i] + more
            spare = spare - more
    return np.array(counts)


def normal_values(rng, dims, scale, reach, split=(), kind=jnp.bfloat16):
    array = scale * jax.random.normal(rng, dims, jnp.float32)
    if split:
        array = array * steps_of(rng, dims, split, -0.22, 0.18)
    return jnp.clip(array, -reach, reach).astype(kind)


def setup_inputs(seed: int = 0, part: int = 0) -> dict:
    splits = jax.random.split(jax.random.key(seed), 7)
    own_keys = jax.random.split(jax.random.fold_in(splits[6], part), 7)
    tokens = normal_values(own_keys[0], (TOKENS, D), 1.0, 6.0, ((0, 4), (1, 4)))
    expert_ids_keys = jax.random.split(jax.random.fold_in(own_keys[1], 1), TOKENS // TOK_EXP)
    expert_ids_turns = jax.random.permutation(jax.random.fold_in(own_keys[1], 3), TOKENS // TOK_EXP)
    expert_ids = jax.vmap(lambda own, number: routed_block(jax.random.fold_in(own_keys[1], 2), own, number, TOK_EXP, EXPERTS, 2, CAP, 2))(expert_ids_keys, expert_ids_turns).reshape((TOKENS, 2))
    route_logits = normal_values(own_keys[2], (TOKENS, 2), 1.5, 6.0, ((0, 4),), jnp.float32)
    gate_weight = normal_values(splits[3], (D, EXPERTS * FF), D ** -0.5, 0.078125, ((1, 16),))
    up_weight = normal_values(splits[4], (D, EXPERTS * FF), D ** -0.5, 0.078125, ((1, 16),))
    down_weight = normal_values(splits[5], (EXPERTS * FF, D), FF ** -0.5, 0.0625, ((0, 16),))
    return {"tokens": tokens, "expert_ids": expert_ids, "route_logits": route_logits, "gate_weight": gate_weight, "up_weight": up_weight, "down_weight": down_weight}


def slot_tables(expert_ids, route_logits):
    chosen = (expert_ids[:, :, None] == jnp.arange(EXPERTS, dtype=jnp.int32)[None, None, :]).astype(jnp.int32)
    per_token = jnp.sum(chosen, axis=1)
    before = jnp.cumsum(per_token, axis=0) - per_token
    position = jnp.sum(chosen * before[:, None, :], axis=2)
    at_slot = (position[:, :, None] == jnp.arange(CAP, dtype=jnp.int32)[None, None, :]).astype(jnp.float32)
    chosen_f = chosen.astype(jnp.float32)
    diff = route_logits[:, 0] - route_logits[:, 1]
    shares = jnp.stack([jax.nn.sigmoid(diff), jax.nn.sigmoid(-diff)], axis=1)
    placement = jnp.einsum('tke,tkc->ect', chosen_f, at_slot)
    mixing = jnp.einsum('tk,tke,tkc->tec', shares, chosen_f, at_slot)
    return placement, mixing


def reference(tokens, expert_ids, route_logits, gate_weight, up_weight, down_weight):
    homes = tokens.reshape(N_EXP, TOK_EXP, D)
    placement, mixing = jax.vmap(slot_tables)(expert_ids.reshape(N_EXP, TOK_EXP, 2), route_logits.reshape(N_EXP, TOK_EXP, 2))
    slots = jnp.einsum('hect,htd->ehcd', placement.astype(jnp.float32), homes.astype(jnp.float32)).astype(jnp.bfloat16)
    block_width = FF // (N_EXP // EXPERTS * N_TP)
    blocks = FF // block_width
    outputs = []
    for expert in range(EXPERTS):
        slot_rows = slots[expert].reshape(N_EXP * CAP, D)
        gate_act = jnp.dot(slot_rows, gate_weight[:, expert * FF:(expert + 1) * FF], preferred_element_type=jnp.float32)
        up_act = jnp.dot(slot_rows, up_weight[:, expert * FF:(expert + 1) * FF], preferred_element_type=jnp.float32)
        hidden = (jax.nn.silu(gate_act) * up_act).astype(jnp.bfloat16)
        hidden_blocks = jnp.transpose(hidden.reshape(N_EXP * CAP, blocks, block_width), (1, 0, 2))
        down_blocks = down_weight[expert * FF:(expert + 1) * FF].reshape(blocks, block_width, D)

        def add_block(running, piece_pair):
            term = jnp.dot(piece_pair[0], piece_pair[1], preferred_element_type=jnp.float32).astype(jnp.bfloat16)
            term = lax.optimization_barrier(term)
            return running + term.astype(jnp.float32), 0

        start = jnp.zeros((N_EXP * CAP, D), jnp.float32)
        summed, unused = lax.scan(add_block, start, (hidden_blocks, down_blocks))
        outputs.append(summed.reshape(N_EXP, CAP, D))
    expert_out = jnp.stack(outputs, axis=0)
    moe_out = jnp.einsum('htec,ehcd->htd', mixing, expert_out, precision=lax.Precision.HIGHEST)
    return moe_out.reshape(TOKENS, D).astype(jnp.bfloat16)
```

```python
import functools

import jax
import jax.numpy as jnp
from jax import lax
from jax.experimental import pallas as pl
from jax.experimental.pallas import tpu as pltpu
from jax.sharding import PartitionSpec as P

EXPERTS = 4
CORES = 2
MESH = pl.DeviceIdType.MESH
F32 = jnp.float32
BF16 = jnp.bfloat16
RING_BYTES = 52 * 1000 * 1000
LAG_PAIR = 2
LAG_HOME = 6
LAG_GATE = 10


class Plan:
    def __init__(self, n_exp, n_tp, tok, dc, width):
        self.n_exp, self.n_tp, self.tok, self.dc, self.width = n_exp, n_tp, tok, dc, width
        self.n_x = n_exp // CORES
        self.h = n_tp // 2
        self.half = self.n_x * tok
        self.lanes = next(t for t in (512, 256, 128) if width % t == 0 and dc % t == 0)
        self.nt = width // self.lanes
        self.group = 2 if self.nt % 2 == 0 else 1
        self.pw = self.lanes if dc > 512 else dc
        self.nq = dc // self.pw
        self.n_pc = n_tp * self.nq
        self.cuts = 2 if tok % 32 == 0 and tok * dc >= 32768 else 1
        self.cut = tok // self.cuts
        loads = []
        steps = self.nt // self.group
        for i in range(n_tp):
            for t in range(self.nt):
                for kind in ("gate", "up"):
                    loads.append((kind, i, t, dc, i * steps + t // self.group))
        for pc in range(self.n_pc):
            i = n_tp - 1 - pc // self.nq
            for t in range(self.pw // self.lanes):
                tile = (pc % self.nq) * (self.pw // self.lanes) + t
                loads.append(("down", i, tile, width, n_tp * steps + pc))
        total = sum(l[3] for l in loads)
        self.rows = min(total, RING_BYTES // (2 * self.lanes) // 16 * 16)
        self.loads, live, head, last = [], [], 0, 0
        for kind, i, t, n, step in loads:
            if head + n > self.rows:
                head = 0
            hit = [l for l in live if l[0] < head + n and head < l[1]]
            last = max([last] + [l[2] + 1 for l in hit])
            assert last <= step
            live = [l for l in live if l not in hit] + [(head, head + n, step)]
            self.loads.append((kind, i, t, n, head, last))
            head += n
        self.at = {l[:3]: n for n, l in enumerate(self.loads)}


def kernel(
    pn,
    tok_hbm,
    ids_hbm,
    log_hbm,
    gate_hbm,
    up_hbm,
    down_hbm,
    out_ref,
    ring,
    rows,
    ids_v,
    log_v,
    shr,
    wcol,
    acc_g,
    acc_u,
    hidden,
    pown,
    psend,
    precv,
    xsend,
    xrecv,
    zsend,
    grecv,
    zrecv,
    gsum,
    own,
    w_sem,
    t_sem,
    rz,
    rx,
    rd,
    s_own,
    s_cross,
    s_fwd,
    sx,
    sd,
    share_x,
    share_d,
    pair2,
    x2,
    sz2,
    rg2,
    rz2,
):
    n_x, n_tp, h, tok, dc = pn.n_x, pn.n_tp, pn.h, pn.tok, pn.dc
    half, nq, lanes, pw = pn.half, pn.nq, pn.lanes, pn.pw
    me = lax.axis_index("exp")
    z = lax.axis_index("tp")
    x = me // CORES
    core = me % CORES
    partner = {"exp": x * CORES + (1 - core)}
    slot = [x] + [lax.rem(x + k, n_x) for k in range(1, n_x)]
    peers = [{"exp": p * CORES + core} for p in slot[1:]]
    side = z // h
    m = z + side * (n_tp - 1 - 2 * z)
    gate = m == h - 1
    member = m != h - 1

    def along(j):
        return {"tp": j + side * (n_tp - 1 - 2 * j)}

    def chunk(i):
        return lax.rem(m + i, h) if i < h else i

    def feature(i):
        return along(chunk(i))["tp"]

    def span(p):
        return pl.ds(pl.multiple_of(p * tok, tok), tok)

    def part(p, c):
        return pl.ds(pl.multiple_of(p * tok + c * pn.cut, pn.cut), pn.cut)

    def remote(src, dst, send, recv, device):
        return pltpu.make_async_remote_copy(
            src_ref=src,
            dst_ref=dst,
            send_sem=send,
            recv_sem=recv,
            device_id=device,
            device_id_type=MESH,
        )

    def load(n):
        kind, i, t, size, at, _ = pn.loads[n]
        f = feature(i)
        if kind == "down":
            c = pl.ds(pl.multiple_of(f * dc + t * lanes, lanes), lanes)
            src = down_hbm.at[:, c]
        else:
            r = pl.ds(pl.multiple_of(f * dc, dc), dc)
            hbm = gate_hbm if kind == "gate" else up_hbm
            src = hbm.at[r, pl.ds(t * lanes, lanes)]
        return pltpu.make_async_copy(src, ring.at[pl.ds(at, size), :], w_sem.at[n])

    def tile(kind, i, t):
        size, at = pn.loads[pn.at[kind, i, t]][3:5]
        return ring[at : at + size, :]

    def start_loads(step):
        for n, l in enumerate(pn.loads):
            if l[5] == step:
                load(n).start()

    sends, gate_sends, member_sends = [], [], []

    def send(copy, log=sends):
        copy.start()
        log.append(copy)

    barrier = pltpu.get_barrier_semaphore()

    def signal(device):
        pl.semaphore_signal(barrier, inc=1, device_id=device, device_id_type=MESH)

    first = [
        pltpu.make_async_copy(ids_hbm, ids_v, t_sem.at[0]),
        pltpu.make_async_copy(log_hbm, log_v, t_sem.at[1]),
        pltpu.make_async_copy(tok_hbm, rows.at[0, span(x), :], t_sem.at[2]),
    ]
    for c in first:
        c.start()
    signal(partner)
    for p in peers:
        signal(p)
    for k in range(1, h):
        signal(along(lax.rem(m + k, h)))
    signal(along(h))

    @pl.when(gate)
    def _():
        for j in range(h + 1, n_tp):
            signal(along(j))

    start_loads(0)

    first[0].wait()
    first[1].wait()
    diff = log_v[0:1, :] - log_v[1:2, :]
    to_first, to_second = jax.nn.sigmoid(diff), jax.nn.sigmoid(-diff)
    for e in range(EXPERTS):
        shr[0, x, e : e + 1, 0:tok] = jnp.where(ids_v[0:1, :] == e, to_first, 0.0) + jnp.where(
            ids_v[1:2, :] == e, to_second, 0.0
        )
    first[2].wait()
    pl.semaphore_wait(barrier, 1 + (n_x - 1) + h + m // max(h - 1, 1) * (h - 1))

    def to_pair(i, p, c):
        return remote(
            rows.at[i, part(slot[p], c), :],
            rows.at[i, pl.ds(pl.multiple_of(half + slot[p] * tok + c * pn.cut, pn.cut), pn.cut), :],
            sd.at[i, p, c],
            rd.at[i, p, c],
            partner,
        )

    def to_peer(i, k, c):
        r = rows.at[i, part(x, c), :]
        return remote(r, r, sx.at[i, k, c], rx.at[i, k, c], peers[k])

    def to_mate(k, c):
        r = part(x, c)
        return remote(
            rows.at[0, r, :], rows.at[h - k, r, :], s_own.at[k, c], rz.at[h - k, c],
            along(lax.rem(m + k, h)),
        )

    def to_cross(c):
        r = part(x, c)
        i = n_tp - 1 - m
        return remote(rows.at[0, r, :], rows.at[i, r, :], s_cross.at[c], rz.at[i, c], along(h))

    def to_member(i, k, c):
        r = rows.at[i, part(x, c), :]
        return remote(r, r, s_fwd.at[i - h, k, c], rz.at[i, c], along(lax.rem(m + k, h)))

    def share_peer(k):
        r = shr.at[0, x]
        return remote(r, r, share_x.at[0, k], share_x.at[1, k], peers[k])

    def share_pair(p):
        return remote(
            shr.at[0, slot[p]], shr.at[1, slot[p]], share_d.at[0, p], share_d.at[1, p], partner
        )

    def spread(i, c):
        for k in range(n_x - 1):
            send(to_peer(i, k, c))
        send(to_pair(i, 0, c))

    def from_line(i, c, log=sends):
        remote_wait = to_member(i, 1, c) if i >= h and h > 1 else None
        r = rows.at[i, part(x, c), :]
        copy = remote_wait or remote(r, r, s_cross.at[c], rz.at[i, c], along(h))
        copy.wait_recv()
        for k in range(n_x - 1):
            to_peer(i, k, c).start()
        to_pair(i, 0, c).start()

    def from_line_at(i, c, who):
        if who == "all":
            from_line(i, c)
        elif who == "gate":

            @pl.when(gate)
            def _():
                r = rows.at[i, part(x, c), :]
                remote(r, r, s_cross.at[c], rz.at[i, c], along(h)).wait_recv()
                for k in range(1, h):
                    to_member(i, k, c).start()
                for k in range(n_x - 1):
                    to_peer(i, k, c).start()
                to_pair(i, 0, c).start()

        elif h > 1:

            @pl.when(member)
            def _():
                from_line(i, c)

    def from_peers(i, c):
        for k in range(n_x - 1):
            to_peer(i, k, c).wait_recv()
            send(to_pair(i, n_x - 1 - k, c))

    for c in range(pn.cuts):
        for k in range(1, h):
            send(to_mate(k, c))
        spread(0, c)
    for c in range(pn.cuts):
        send(to_cross(c))
    for k in range(n_x - 1):
        send(share_peer(k))
    send(share_pair(0))

    arrivals = {s: [] for s in range(-1, n_tp)}
    for i in range(n_tp):
        if i >= h:
            arrivals[max(i - 3, -1)].append((0, i, "gate"))
        if i > 0:
            arrivals[max(i - 2, -1)].append((1 if i < h else 3, i, "all" if i < h else "member"))
        arrivals[i - 1].append((2, i, "peers"))

    def arrive(s, c):
        for _, i, who in sorted(arrivals[s], key=lambda a: (a[0] != 1, a[0], a[1])):
            if who == "peers":
                from_peers(i, c)
            else:
                from_line_at(i, c, who)

    for c in range(pn.cuts):
        arrive(-1, c)

    ngroups = pn.nt // pn.group
    groups_of = n_tp * ngroups
    for i in range(n_tp):
        for p in range(n_x):
            for c in range(pn.cuts):
                to_pair(i, p, c).wait_recv()
        if i == n_tp - 1:
            for k in range(n_x - 1):
                share_peer(k).wait_recv()
                send(share_pair(n_x - 1 - k))
            for p in range(n_x):
                share_pair(p).wait_recv()
            expert = me // (pn.n_exp // EXPERTS)
            eye = lax.broadcasted_iota(jnp.int32, (tok, tok), 0) == lax.broadcasted_iota(
                jnp.int32, (tok, tok), 1
            )
            for side_of in range(CORES):
                for p in range(n_x):
                    row = shr[side_of, p, pl.ds(expert, 1), 0:tok]
                    col = jnp.sum(
                        jnp.where(eye, jnp.broadcast_to(row, (tok, tok)), 0.0), axis=1, keepdims=True
                    )
                    at = side_of * half + p * tok
                    wcol[at : at + tok, :] = jnp.broadcast_to(col, (tok, 128))
        for g in range(ngroups):
            tiles = range(g * pn.group, (g + 1) * pn.group)
            for t in tiles:
                load(pn.at["gate", i, t]).wait()
                load(pn.at["up", i, t]).wait()
            for t in tiles:
                cols = slice(t * lanes, (t + 1) * lanes)
                a = rows[i]
                gv = jnp.dot(a, tile("gate", i, t), preferred_element_type=F32)
                uv = jnp.dot(a, tile("up", i, t), preferred_element_type=F32)
                if i > 0:
                    gv = gv + acc_g[:, cols]
                    uv = uv + acc_u[:, cols]
                if i < n_tp - 1:
                    acc_g[:, cols] = gv
                    acc_u[:, cols] = uv
                else:
                    hidden[:, cols] = (gv * jax.nn.sigmoid(gv) * uv * wcol[:, 0:1]).astype(BF16)
            start_loads(i * ngroups + g + 1)
            if i < n_tp - 1:
                for c in range(pn.cuts):
                    if min(c, ngroups - 1) == g or (g == ngroups - 1 and c >= ngroups):
                        arrive(i, c)

    n_pc = pn.n_pc
    n_cross = h * nq

    def pair_of(pc):
        return remote(psend.at[pc], precv.at[pc], pair2.at[0, pc], pair2.at[1, pc], partner)

    def x_of(pc, k):
        return remote(
            xsend.at[pc, k], xrecv.at[pc, k], x2.at[0, pc, k], x2.at[1, pc, k], peers[k]
        )

    def place(pc):
        return n_tp - 1 - pc // nq, pc % nq

    def to_gateway(pc):
        return remote(
            zsend.at[pc], grecv.at[m, pc], sz2.at[pc], rg2.at[m, pc], along(h - 1)
        )

    def from_member(mm, pc):
        return remote(
            zsend.at[pc], grecv.at[mm, pc], sz2.at[pc], rg2.at[mm, pc], along(h - 1)
        )

    def to_dest(pc):
        i, q = place(pc)
        r = 0 if i >= h else i
        return remote(zsend.at[pc], zrecv.at[r, q], sz2.at[pc], rz2.at[r, q], along(chunk(i)))

    def compute(pc):
        i, q = place(pc)
        for t in range(pw // lanes):
            n = q * (pw // lanes) + t
            load(pn.at["down", i, n]).wait()
            cols = slice(t * lanes, (t + 1) * lanes)
            p = jnp.dot(hidden[...], tile("down", i, n), preferred_element_type=F32)
            pown[pc, :, cols] = p[:half]
            psend[pc, :, cols] = p[half:].astype(BF16)
        start_loads(groups_of + pc + 1)
        send(pair_of(pc))

    def combine(pc):
        pair_of(pc).wait_recv()
        for k in range(n_x - 1):
            r = span(slot[k + 1])
            xsend[pc, k] = (pown[pc, r, :] + precv[pc, r, :].astype(F32)).astype(BF16)
            send(x_of(pc, k))

    def home(pc):
        i, q = place(pc)
        r = span(x)
        total = pown[pc, r, :] + precv[pc, r, :].astype(F32)
        for k in range(n_x - 1):
            x_of(pc, k).wait_recv()
            total = total + xrecv[pc, k].astype(F32)
        if i == 0:
            own[q] = total
        elif i < h:
            zsend[pc] = total.astype(BF16)
            send(to_dest(pc))
        else:
            if h > 1:

                @pl.when(member)
                def _():
                    zsend[pc] = total.astype(BF16)
                    to_gateway(pc).start()

            @pl.when(gate)
            def _():
                gsum[pc] = total

    def relay(pc):
        @pl.when(gate)
        def _():
            total = gsum[pc]
            for mm in range(h - 1):
                from_member(mm, pc).wait_recv()
                total = total + grecv[mm, pc].astype(F32)
            zsend[pc] = total.astype(BF16)
            to_dest(pc).start()

    for s in range(n_pc + max(LAG_PAIR, LAG_HOME, LAG_GATE)):
        if s < n_pc:
            compute(s)
        if 0 <= s - LAG_PAIR < n_pc:
            combine(s - LAG_PAIR)
        if 0 <= s - LAG_HOME < n_pc:
            home(s - LAG_HOME)
        if 0 <= s - LAG_GATE < n_cross:
            relay(s - LAG_GATE)
    for q in range(nq):
        total = own[q]
        for r in range(1, h):
            to_dest((n_tp - 1 - r) * nq + q).wait_recv()
            total = total + zrecv[r, q].astype(F32)
        to_dest(q).wait_recv()
        total = total + zrecv[0, q].astype(F32)
        out_ref[:, q * pw : (q + 1) * pw] = total.astype(BF16)

    for c in sends:
        c.wait_send()
    for i in range(1, n_tp):
        for c in range(pn.cuts):
            for k in range(n_x - 1):
                to_peer(i, k, c).wait_send()
            to_pair(i, 0, c).wait_send()
    for pc in range(n_cross):
        to_dest(pc).wait_send()

    @pl.when(gate)
    def _():
        for i in range(h, n_tp):
            for k in range(1, h):
                for c in range(pn.cuts):
                    to_member(i, k, c).wait_send()


def on_device(tokens, expert_ids, route_logits, gate_weight, up_weight, down_weight):
    n_exp = lax.axis_size("exp")
    n_tp = lax.axis_size("tp")
    tok, dc = tokens.shape
    width = gate_weight.shape[1]
    pn = Plan(n_exp, n_tp, tok, dc, width)
    n_x, h, half, nq, n_pc, pw = pn.n_x, pn.h, pn.half, pn.nq, pn.n_pc, pn.pw
    total = n_exp * tok
    mates = max(h - 1, 1)
    peers = max(n_x - 1, 1)
    dma = pltpu.SemaphoreType.DMA
    hbm = pl.BlockSpec(memory_space=pl.ANY)
    return pl.pallas_call(
        functools.partial(kernel, pn),
        out_shape=pltpu.VMEM((tok, dc), BF16),
        in_specs=[hbm] * 6,
        out_specs=pl.BlockSpec(memory_space=pltpu.VMEM),
        scratch_shapes=[
            pltpu.VMEM((pn.rows, pn.lanes), BF16),
            pltpu.VMEM((n_tp, total, dc), BF16),
            pltpu.VMEM((2, tok), jnp.int32),
            pltpu.VMEM((2, tok), F32),
            pltpu.VMEM((CORES, n_x, 8, 128), F32),
            pltpu.VMEM((total, 128), F32),
            pltpu.VMEM((total, width), F32),
            pltpu.VMEM((total, width), F32),
            pltpu.VMEM((total, width), BF16),
            pltpu.VMEM((n_pc, half, pw), F32),
            pltpu.VMEM((n_pc, half, pw), BF16),
            pltpu.VMEM((n_pc, half, pw), BF16),
            pltpu.VMEM((n_pc, peers, tok, pw), BF16),
            pltpu.VMEM((n_pc, peers, tok, pw), BF16),
            pltpu.VMEM((n_pc, tok, pw), BF16),
            pltpu.VMEM((mates, h * nq, tok, pw), BF16),
            pltpu.VMEM((h, nq, tok, pw), BF16),
            pltpu.VMEM((h * nq, tok, pw), F32),
            pltpu.VMEM((nq, tok, pw), F32),
            dma((len(pn.loads),)),
            dma((3,)),
            dma((n_tp, pn.cuts)),
            dma((n_tp, peers, pn.cuts)),
            dma((n_tp, n_x, pn.cuts)),
            dma((h, pn.cuts)),
            dma((pn.cuts,)),
            dma((h, h, pn.cuts)),
            dma((n_tp, peers, pn.cuts)),
            dma((n_tp, n_x, pn.cuts)),
            dma((2, peers)),
            dma((2, n_x)),
            dma((2, n_pc)),
            dma((2, n_pc, peers)),
            dma((n_pc,)),
            dma((mates, h * nq)),
            dma((h, nq)),
        ],
        compiler_params=pltpu.CompilerParams(
            collective_id=0, has_side_effects=True, vmem_limit_bytes=66500000
        ),
    )(tokens, expert_ids.T, route_logits.T, gate_weight, up_weight, down_weight)


def solution(mesh):
    return jax.shard_map(
        on_device,
        mesh=mesh,
        in_specs=(
            P(("rep", "exp"), "tp"),
            P(("rep", "exp"), None),
            P(("rep", "exp"), None),
            P(None, ("exp", "tp")),
            P(None, ("exp", "tp")),
            P(("exp", "tp"), None),
        ),
        out_specs=P(("rep", "exp"), "tp"),
        check_vma=False,
    )
```
